32 devices in a mesh: dp: 2 (over x), row: 4 (over y, core), col: 4 (over z).
Axes of the slice: x: 2, y: 2, z: 4, core: 2. Of those that a mesh axis runs over, the one named last changes fastest.
Arguments:
- tokens: bfloat16 [512, 4608], P(('dp', 'row'), 'col'), may hold values from -6 to 6
- cotangent: bfloat16 [512, 4608], P(('dp', 'row'), 'col'), may hold values from -3 to 3
- w_gate: bfloat16 [36864, 4608], P(('dp', 'row'), 'col'), may hold values from -0.09375 to 0.09375
- w_up: bfloat16 [36864, 4608], P(('dp', 'row'), 'col'), may hold values from -0.09375 to 0.09375
- w_down: bfloat16 [36864, 4608], P(('dp', 'row'), 'col'), may hold values from -0.03125 to 0.03125
Outputs:
- grad_tokens: bfloat16 [512, 4608], P(('dp', 'row'), 'col')
- grad_w_gate: float32 [36864, 4608], P(('dp', 'row'), 'col')
- grad_w_up: float32 [36864, 4608], P(('dp', 'row'), 'col')
- grad_w_down: float32 [36864, 4608], P(('dp', 'row'), 'col')
The draws below stay inside these ranges and needn't reach their ends.
All inputs are finite; a program needn't handle non-finite values.
Results may differ from the reference program's by a relative error of at most 0.003.
Values may be sent and summed in bfloat16 or wider, within the bound.
A program may use at most 320 MiB of HBM per device.

```python
import math
import jax
import jax.numpy as jnp
from jax import lax

D = 4608
FF = 36864
GROUPS = 4
TOKENS = 512


def levels(rng, extent, split, least, top_value):
    factor_of = 1.0
    for dim, blocks in split:
        steps = jax.random.uniform(jax.random.fold_in(jax.random.fold_in(rng, 6), dim), (blocks,), jnp.float32, least / len(split), top_value / len(split))
        factor_of = factor_of * jnp.repeat(jnp.exp(steps), extent[dim] // blocks).reshape((-1,) + (1,) * (len(extent) - 1 - dim))
    return factor_of


def normal_values(stream_key, dims, spread, limit, pieces=(), dtype=jnp.bfloat16):
    entries = jax.random.normal(stream_key, dims, jnp.float32) * spread
    if len(pieces) > 0:
        entries = levels(stream_key, dims, pieces, -0.22, 0.18) * entries
    return jnp.clip(entries, min=-limit, max=limit).astype(dtype)


def setup_inputs(seed: int = 0) -> dict:
    key_list = jax.random.split(jax.random.key(seed), 6)
    tokens = normal_values(key_list[0], (TOKENS, D), 1.0, 6.0, ((0, 8), (1, 4)))
    cotangent = normal_values(key_list[1], (TOKENS, D), 0.5, 3.0, ((0, 8), (1, 4)))
    w_gate = normal_values(key_list[2], (FF, D), D ** -0.5, 0.09375, ((0, 8), (1, 4)))
    w_up = normal_values(key_list[3], (FF, D), D ** -0.5, 0.09375, ((0, 8), (1, 4)))
    w_down = normal_values(key_list[4], (FF, D), FF ** -0.5, 0.03125, ((0, 8), (1, 4)))
    return dict(tokens=tokens, cotangent=cotangent, w_gate=w_gate, w_up=w_up, w_down=w_down)


gelu_scale = math.sqrt(2.0 / math.pi)
cubic_coeff = 0.044715

def gelu_parts(pre_gate):
    tanh_arg = gelu_scale * (pre_gate + cubic_coeff * pre_gate * pre_gate * pre_gate)
    tanh_val = jnp.tanh(tanh_arg)
    gelu_out = 0.5 * pre_gate * (1.0 + tanh_val)
    gelu_slope = 0.5 * (1.0 + tanh_val) + 0.5 * pre_gate * (1.0 - tanh_val * tanh_val) * gelu_scale * (1.0 + 3.0 * cubic_coeff * pre_gate * pre_gate)
    return (gelu_out, gelu_slope)

def pointwise(pre_gate, pre_up, grad_hidden):
    gelu_out, gelu_slope = gelu_parts(pre_gate)
    hidden = (gelu_out * pre_up).astype(jnp.bfloat16)
    grad_gate = (grad_hidden * pre_up * gelu_slope).astype(jnp.bfloat16)
    grad_up = (grad_hidden * gelu_out).astype(jnp.bfloat16)
    return (hidden, grad_gate, grad_up)

def rounded_sum(first_op, second_op):
    partial_sum = jnp.dot(first_op.T, second_op, preferred_element_type=jnp.float32)
    return lax.optimization_barrier(partial_sum.astype(jnp.bfloat16)).astype(jnp.float32)

def reference(tokens, cotangent, w_gate, w_up, w_down):
    pre_gate = jnp.dot(tokens, w_gate.T, preferred_element_type=jnp.float32)
    pre_up = jnp.dot(tokens, w_up.T, preferred_element_type=jnp.float32)
    grad_hidden = jnp.dot(cotangent, w_down.T, preferred_element_type=jnp.float32)
    hidden, grad_gate, grad_up = pointwise(pre_gate, pre_up, grad_hidden)
    grad_in = jnp.dot(grad_gate, w_gate, preferred_element_type=jnp.float32) + jnp.dot(grad_up, w_up, preferred_element_type=jnp.float32)
    grad_in = grad_in.astype(jnp.bfloat16)
    group_rows = TOKENS // GROUPS
    gate_grad = jnp.zeros(w_gate.shape, jnp.float32)
    up_grad = jnp.zeros(w_up.shape, jnp.float32)
    down_grad = jnp.zeros(w_down.shape, jnp.float32)
    for group in range(GROUPS):
        first_row = group * group_rows
        tok_block = tokens[first_row:first_row + group_rows]
        cot_block = cotangent[first_row:first_row + group_rows]
        gate_grad = gate_grad + rounded_sum(grad_gate[first_row:first_row + group_rows], tok_block)
        up_grad = up_grad + rounded_sum(grad_up[first_row:first_row + group_rows], tok_block)
        down_grad = down_grad + rounded_sum(hidden[first_row:first_row + group_rows], cot_block)
    return (grad_in, gate_grad, up_grad, down_grad)
```

```python
import math

import jax
import jax.numpy as jnp
from jax import lax
from jax.experimental import pallas as pl
from jax.experimental.pallas import tpu as pltpu
from jax.sharding import PartitionSpec as P

GROUPS = 4
BLOCKS = 4
BF, HF, F32 = jnp.bfloat16, jnp.float16, jnp.float32

gelu_scale = math.sqrt(2.0 / math.pi)
cubic_coeff = 0.044715


def gelu_parts(pre_gate):
    tanh_arg = gelu_scale * (pre_gate + cubic_coeff * pre_gate * pre_gate * pre_gate)
    tanh_val = jnp.tanh(tanh_arg)
    gelu_out = 0.5 * pre_gate * (1.0 + tanh_val)
    gelu_slope = 0.5 * (1.0 + tanh_val) + 0.5 * pre_gate * (
        1.0 - tanh_val * tanh_val
    ) * gelu_scale * (1.0 + 3.0 * cubic_coeff * pre_gate * pre_gate)
    return (gelu_out, gelu_slope)


def pointwise(pre_gate, pre_up, grad_hidden):
    gelu_out, gelu_slope = gelu_parts(pre_gate)
    hidden = (gelu_out * pre_up).astype(BF)
    grad_gate = (grad_hidden * pre_up * gelu_slope).astype(BF)
    grad_up = (grad_hidden * gelu_out).astype(BF)
    return (grad_gate, grad_up, hidden)


def shift(value, axis, by):
    size = lax.axis_size(axis)
    return lax.ppermute(value, axis, [(k, (k + by) % size) for k in range(size)])


def core_swap(value):
    size = lax.axis_size("row")
    return lax.ppermute(value, "row", [(k, k ^ 1) for k in range(size)])


def chip_swap(value, axis):
    size = lax.axis_size(axis)
    return lax.ppermute(value, axis, [(k, (k + size // 2) % size) for k in range(size)])


def ordered(mine, other, bit):
    low = jnp.where(bit == 0, mine, other)
    high = jnp.where(bit == 0, other, mine)
    return low, high


def gather_rows(x):
    if lax.axis_size("dp") != 2 or lax.axis_size("row") != 4:
        return lax.all_gather(x, ("dp", "row"), axis=1, tiled=True)
    dp, row = lax.axis_index("dp"), lax.axis_index("row")
    y, core = row // 2, row % 2
    first, second = x[0], x[1]
    fy = jnp.stack(ordered(first, chip_swap(first, "row"), y), 0)
    sx = jnp.stack(ordered(second, chip_swap(second, "dp"), dp), 0)
    fxy = jnp.stack(ordered(fy, chip_swap(fy, "dp"), dp), 0)
    sxy = jnp.stack(ordered(sx, chip_swap(sx, "row"), y), 1)
    both = jnp.stack((fxy, sxy), 0)
    low, high = ordered(both, core_swap(both), core)
    full = jnp.stack((low, high), 3)
    return full.reshape(2, -1, x.shape[2])


def scatter_rows(x):
    if lax.axis_size("dp") != 2 or lax.axis_size("row") != 4:
        return lax.psum_scatter(x, ("dp", "row"), scatter_dimension=0, tiled=True)
    dp, row = lax.axis_index("dp"), lax.axis_index("row")
    y, core = row // 2, row % 2
    rows = x.shape[0] // 8
    half = x.shape[1] // 256 * 128

    def pick(v, dim, index):
        return lax.dynamic_index_in_dim(v, index, dim, keepdims=False)

    v = x.reshape(2, 2, 2, rows, x.shape[1])
    v = pick(v, 2, core) + core_swap(pick(v, 2, 1 - core))
    a, b = v[..., :half], v[..., half:]
    a1 = pick(a, 1, y) + chip_swap(pick(a, 1, 1 - y), "row")
    b1 = pick(b, 0, dp) + chip_swap(pick(b, 0, 1 - dp), "dp")
    a2 = pick(a1, 0, dp) + chip_swap(pick(a1, 0, 1 - dp), "dp")
    b2 = pick(b1, 0, y) + chip_swap(pick(b1, 0, 1 - y), "row")
    return jnp.concatenate((a2, b2), 1)


def grads_kernel(act_ref, tok_ref, cot_ref, *rest):
    outs = rest[-3:]
    rows = tok_ref.shape[0] // GROUPS
    for which, (src, out) in enumerate(zip((tok_ref, tok_ref, cot_ref), outs)):
        total = None
        for group in range(GROUPS):
            span = pl.ds(group * rows, rows)
            part = jnp.dot(act_ref[which, :, span], src[span, :], preferred_element_type=F32)
            part = part.astype(BF).astype(F32)
            total = part if total is None else total + part
        out[...] = total


def weight_grads(act, tok, cot, held, block, ff):
    _, rows, count = act.shape
    features = tok.shape[1]
    tile = next(t for t in (192, 144, 128, 96, 64, 48, 32, 16) if rows % t == 0)
    steps = rows // tile
    whole = pl.BlockSpec((count, features), lambda i: (0, 0))
    out_spec = pl.BlockSpec((tile, features), lambda i: (block * steps + i, 0))
    out_shape = jax.ShapeDtypeStruct((ff, features), F32)
    held_specs = [pl.BlockSpec(memory_space=pl.ANY)] * len(held)
    return pl.pallas_call(
        grads_kernel,
        grid=(steps,),
        in_specs=[pl.BlockSpec((3, tile, count), lambda i: (0, i, 0)), whole, whole] + held_specs,
        out_specs=[out_spec] * 3,
        out_shape=[out_shape] * 3,
        input_output_aliases={3 + k: k for k in range(len(held))},
        cost_estimate=pl.CostEstimate(
            flops=12 * rows * count * features,
            bytes_accessed=12 * rows * features + 6 * rows * count + 4 * count * features,
            transcendentals=0,
        ),
    )(act, tok, cot, *held)


def shards(tokens, cotangent, w_gate, w_up, w_down):
    cols = lax.axis_size("col")
    me = lax.axis_index("col")
    ff, features = w_gate.shape
    weights = (w_gate, w_up, w_down)
    wmax = [jnp.max(jnp.abs(w)).astype(F32) for w in weights]
    rows_all = gather_rows(jnp.stack((tokens, cotangent), 0))
    tok, cot = rows_all[0], rows_all[1]
    count = tok.shape[0]

    amax = [jnp.max(jnp.abs(v)).astype(F32) for v in (tok, cot)]
    peaks = jnp.stack(wmax + amax)
    peaks = jnp.broadcast_to(peaks[:, None], (5, 128))
    for by in (1, 2):
        peaks = jnp.maximum(peaks, shift(peaks, "col", by))
    tops = jnp.maximum(peaks[:, 0], 1e-18)
    bounds = [tops[k] * tops[3 + a] * (features * cols) for k, a in ((0, 0), (1, 0), (2, 1))]
    down_by = [32768.0 / b for b in bounds]
    up_by = [b / 32768.0 for b in bounds]

    fb = ff // BLOCKS
    fc = fb // 4
    fh = fc // 2

    def terms(block, rel, first, rows):
        start = block * fb + ((me + rel) % 4) * fc + first
        out = []
        for w, act, factor in zip(weights, (tok, tok, cot), down_by):
            part = lax.dynamic_slice_in_dim(w, start, rows, 0)
            out.append(
                lax.dot_general(part, act, (((1,), (1,)), ((), ())), preferred_element_type=F32)
                * factor
            )
        return jnp.stack(out, 0)

    def send_block(block):
        far = terms(block, 2, 0, fc).astype(HF)
        right = terms(block, 1, 0, fc)
        left = terms(block, 3, 0, fc)
        r1 = shift(jnp.concatenate((far[:, :fh], right[:, fh:].astype(HF)), 1), "col", 1)
        l1 = shift(jnp.concatenate((left[:, :fh].astype(HF), far[:, fh:]), 1), "col", -1)
        r2 = shift((right[:, :fh] + r1[:, :fh].astype(F32)).astype(HF), "col", 1)
        l2 = shift((left[:, fh:] + l1[:, fh:].astype(F32)).astype(HF), "col", -1)
        own = terms(block, 0, 0, fc)
        low = own[:, :fh] + r2.astype(F32) + l1[:, :fh].astype(F32)
        high = own[:, fh:] + r1[:, fh:].astype(F32) + l2.astype(F32)
        both = jnp.concatenate((low, high), 1)
        return jnp.stack(pointwise(*(both[k] * up_by[k] for k in range(3))), 0)

    def spread(act):
        from_left = shift(act, "col", 1)
        from_right = shift(act, "col", -1)
        far_low = shift(from_left[:, :fh], "col", 1)
        far_high = shift(from_right[:, fh:], "col", -1)
        out = jnp.zeros((3, fb, count), BF)
        for value, rel, first in (
            (act, 0, 0),
            (from_left, 3, 0),
            (from_right, 1, 0),
            (far_low, 2, 0),
            (far_high, 2, fh),
        ):
            out = lax.dynamic_update_slice_in_dim(out, value, ((me + rel) % 4) * fc + first, 1)
        return out

    total = None
    held = ()
    for block in range(BLOCKS):
        if cols == 4:
            act = spread(send_block(block))
        else:
            span = slice(block * fb, (block + 1) * fb)
            pre = tuple(
                lax.dot_general(w[span], a, (((1,), (1,)), ((), ())), preferred_element_type=F32)
                for w, a in zip(weights, (tok, tok, cot))
            )
            act = jnp.stack(pointwise(*lax.psum(pre, "col")), 0)
        span = slice(block * fb, (block + 1) * fb)
        for k in range(2):
            term = lax.dot_general(
                act[k], weights[k][span], (((0,), (0,)), ((), ())), preferred_element_type=F32
            )
            total = term if total is None else total + term
        held = weight_grads(act, tok, cot, held, block, ff)
    grad_in = scatter_rows(total)
    return (grad_in.astype(BF), *held)


def solution(mesh):
    spec = P(("dp", "row"), "col")
    return jax.shard_map(
        shards,
        mesh=mesh,
        in_specs=(spec,) * 5,
        out_specs=(spec,) * 4,
        check_vma=False,
    )
```

```python
import math

import jax
import jax.numpy as jnp
from jax import lax
from jax.experimental import pallas as pl
from jax.experimental.pallas import tpu as pltpu
from jax.sharding import PartitionSpec as P

GROUPS = 4
BLOCKS = 4
BF, HF, F32 = jnp.bfloat16, jnp.float16, jnp.float32

gelu_scale = math.sqrt(2.0 / math.pi)
cubic_coeff = 0.044715


def gelu_parts(pre_gate):
    tanh_arg = gelu_scale * (pre_gate + cubic_coeff * pre_gate * pre_gate * pre_gate)
    tanh_val = jnp.tanh(tanh_arg)
    gelu_out = 0.5 * pre_gate * (1.0 + tanh_val)
    gelu_slope = 0.5 * (1.0 + tanh_val) + 0.5 * pre_gate * (
        1.0 - tanh_val * tanh_val
    ) * gelu_scale * (1.0 + 3.0 * cubic_coeff * pre_gate * pre_gate)
    return (gelu_out, gelu_slope)


def pointwise(pre_gate, pre_up, grad_hidden):
    gelu_out, gelu_slope = gelu_parts(pre_gate)
    hidden = (gelu_out * pre_up).astype(BF)
    grad_gate = (grad_hidden * pre_up * gelu_slope).astype(BF)
    grad_up = (grad_hidden * gelu_out).astype(BF)
    return (grad_gate, grad_up, hidden)


def shift(value, axis, by):
    size = lax.axis_size(axis)
    return lax.ppermute(value, axis, [(k, (k + by) % size) for k in range(size)])


def core_swap(value):
    size = lax.axis_size("row")
    return lax.ppermute(value, "row", [(k, k ^ 1) for k in range(size)])


def chip_swap(value, axis):
    size = lax.axis_size(axis)
    return lax.ppermute(value, axis, [(k, (k + size // 2) % size) for k in range(size)])


def ordered(mine, other, bit):
    low = jnp.where(bit == 0, mine, other)
    high = jnp.where(bit == 0, other, mine)
    return low, high


def gather_rows(x):
    if lax.axis_size("dp") != 2 or lax.axis_size("row") != 4:
        return lax.all_gather(x, ("dp", "row"), axis=1, tiled=True)
    dp, row = lax.axis_index("dp"), lax.axis_index("row")
    y, core = row // 2, row % 2
    first, second = x[0], x[1]
    fy = jnp.stack(ordered(first, chip_swap(first, "row"), y), 0)
    sx = jnp.stack(ordered(second, chip_swap(second, "dp"), dp), 0)
    fxy = jnp.stack(ordered(fy, chip_swap(fy, "dp"), dp), 0)
    sxy = jnp.stack(ordered(sx, chip_swap(sx, "row"), y), 1)
    both = jnp.stack((fxy, sxy), 0)
    low, high = ordered(both, core_swap(both), core)
    full = jnp.stack((low, high), 3)
    return full.reshape(2, -1, x.shape[2])


def scatter_rows(x):
    if lax.axis_size("dp") != 2 or lax.axis_size("row") != 4:
        return lax.psum_scatter(x, ("dp", "row"), scatter_dimension=0, tiled=True)
    dp, row = lax.axis_index("dp"), lax.axis_index("row")
    y, core = row // 2, row % 2
    rows = x.shape[0] // 8
    half = x.shape[1] // 256 * 128

    def pick(v, dim, index):
        return lax.dynamic_index_in_dim(v, index, dim, keepdims=False)

    v = x.reshape(2, 2, 2, rows, x.shape[1])
    v = pick(v, 2, core) + core_swap(pick(v, 2, 1 - core))
    a, b = v[..., :half], v[..., half:]
    a1 = pick(a, 1, y) + chip_swap(pick(a, 1, 1 - y), "row")
    b1 = pick(b, 0, dp) + chip_swap(pick(b, 0, 1 - dp), "dp")
    a2 = pick(a1, 0, dp) + chip_swap(pick(a1, 0, 1 - dp), "dp")
    b2 = pick(b1, 0, y) + chip_swap(pick(b1, 0, 1 - y), "row")
    return jnp.concatenate((a2, b2), 1)


def grads_kernel(act_ref, tok_ref, cot_ref, *rest):
    outs = rest[-3:]
    rows = tok_ref.shape[0] // GROUPS
    for which, (src, out) in enumerate(zip((tok_ref, tok_ref, cot_ref), outs)):
        total = None
        for group in range(GROUPS):
            span = pl.ds(group * rows, rows)
            part = jnp.dot(act_ref[which, :, span], src[span, :], preferred_element_type=F32)
            part = part.astype(BF).astype(F32)
            total = part if total is None else total + part
        out[...] = total


def weight_grads(act, tok, cot, held, block, ff):
    _, rows, count = act.shape
    features = tok.shape[1]
    tile = next(t for t in (192, 144, 128, 96, 64, 48, 32, 16) if rows % t == 0)
    steps = rows // tile
    whole = pl.BlockSpec((count, features), lambda i: (0, 0))
    out_spec = pl.BlockSpec((tile, features), lambda i: (block * steps + i, 0))
    out_shape = jax.ShapeDtypeStruct((ff, features), F32)
    held_specs = [pl.BlockSpec(memory_space=pl.ANY)] * len(held)
    return pl.pallas_call(
        grads_kernel,
        grid=(steps,),
        in_specs=[pl.BlockSpec((3, tile, count), lambda i: (0, i, 0)), whole, whole] + held_specs,
        out_specs=[out_spec] * 3,
        out_shape=[out_shape] * 3,
        input_output_aliases={3 + k: k for k in range(len(held))},
        cost_estimate=pl.CostEstimate(
            flops=12 * rows * count * features,
            bytes_accessed=12 * rows * features + 6 * rows * count + 4 * count * features,
            transcendentals=0,
        ),
    )(act, tok, cot, *held)


def shards(tokens, cotangent, w_gate, w_up, w_down):
    cols = lax.axis_size("col")
    me = lax.axis_index("col")
    ff, features = w_gate.shape
    weights = (w_gate, w_up, w_down)
    wmax = [jnp.max(jnp.abs(w)).astype(F32) for w in weights]
    rows_all = gather_rows(jnp.stack((tokens, cotangent), 0))
    tok, cot = rows_all[0], rows_all[1]
    count = tok.shape[0]

    amax = [jnp.max(jnp.abs(v)).astype(F32) for v in (tok, cot)]
    peaks = jnp.stack(wmax + amax)
    peaks = jnp.broadcast_to(peaks[:, None], (5, 128))
    for by in (1, 2):
        peaks = jnp.maximum(peaks, shift(peaks, "col", by))
    tops = jnp.maximum(peaks[:, 0], 1e-18)
    bounds = [tops[k] * tops[3 + a] * (features * cols) for k, a in ((0, 0), (1, 0), (2, 1))]
    down_by = [32768.0 / b for b in bounds]
    up_by = [b / 32768.0 for b in bounds]

    fb = ff // BLOCKS
    fc = fb // 4
    fh = fc // 2

    def terms(block, acts):
        start = block * fb
        outs = []
        for w, act, factor in zip(weights, acts, down_by):
            part = lax.slice_in_dim(w, start, start + fb, axis=0)
            outs.append(
                lax.dot_general(part, act, (((1,), (1,)), ((), ())), preferred_element_type=F32)
                * factor
            )
        return [v.astype(HF) for v in outs]

    def rows_of(parts, rel, first, rows):
        start = ((me + rel) % 4) * fc + first
        return jnp.stack([lax.dynamic_slice_in_dim(v, start, rows, 0) for v in parts], 0)

    def first_sends(parts):
        to_right = jnp.concatenate((rows_of(parts, 2, 0, fh), rows_of(parts, 1, fh, fh)), 1)
        to_left = jnp.concatenate((rows_of(parts, 3, 0, fh), rows_of(parts, 2, fh, fh)), 1)
        return to_right, to_left

    def second_sends(parts, r1, l1):
        right, left = rows_of(parts, 1, 0, fh), rows_of(parts, 3, fh, fh)
        to_right = (right.astype(F32) + r1[:, :fh].astype(F32)).astype(HF)
        to_left = (left.astype(F32) + l1[:, fh:].astype(F32)).astype(HF)
        return to_right, to_left

    def own_part(parts, r1, l1, r2, l2):
        own = rows_of(parts, 0, 0, fc).astype(F32)
        low = own[:, :fh] + r2.astype(F32) + l1[:, :fh].astype(F32)
        high = own[:, fh:] + r1[:, fh:].astype(F32) + l2.astype(F32)
        both = jnp.concatenate((low, high), 1)
        return jnp.stack(pointwise(*(both[k] * up_by[k] for k in range(3))), 0)

    def reduced_blocks():
        acts = (tok, tok, cot)
        parts, one, two, done = {}, {}, {}, {}
        for step in range(BLOCKS + 2):
            ready = []
            if step < BLOCKS:
                parts[step] = terms(step, acts)
                sends = first_sends(parts[step])
                ready += sends
                one[step] = (sends, None)
            for table in (one,):
                sends = table.get(step - 1)
                if sends is not None:
                    r1, l1 = shift(sends[0][0], "col", 1), shift(sends[0][1], "col", -1)
                    nxt = second_sends(parts[step - 1], r1, l1)
                    ready += nxt
                    two[step - 1] = (r1, l1, nxt)
            if step - 2 in two:
                r1, l1, nxt = two[step - 2]
                r2, l2 = shift(nxt[0], "col", 1), shift(nxt[1], "col", -1)
                done[step - 2] = own_part(parts[step - 2], r1, l1, r2, l2)
                ready.append(done[step - 2])
            if step + 1 < BLOCKS:
                t, c, *ready = lax.optimization_barrier((acts[0], acts[2], *ready))
                acts = (t, t, c)
                ready = list(ready)
                one[step] = ((ready[0], ready[1]), None)
                if step - 1 in two:
                    r1, l1, _ = two[step - 1]
                    two[step - 1] = (r1, l1, (ready[2], ready[3]))
                if step - 2 in done:
                    done[step - 2] = ready[4]
        return [done[k] for k in range(BLOCKS)]

    def spread(act, after):
        from_left = shift(act, "col", 1)
        from_right = shift(act, "col", -1)
        far_low = shift(from_left[:, :fh], "col", 1)
        far_high = shift(from_right[:, fh:], "col", -1)
        act, *after = lax.optimization_barrier((act, *after))
        out = jnp.zeros((3, fb, count), BF)
        for value, rel, first in (
            (act, 0, 0),
            (from_left, 3, 0),
            (from_right, 1, 0),
            (far_low, 2, 0),
            (far_high, 2, fh),
        ):
            out = lax.dynamic_update_slice_in_dim(out, value, ((me + rel) % 4) * fc + first, 1)
        return out, after

    total = None
    held = ()
    reduced = reduced_blocks() if cols == 4 else ()
    for block in range(BLOCKS):
        if cols == 4:
            after = () if total is None else (total, *held)
            act, after = spread(reduced[block], after)
            if after:
                total, *held = after
        else:
            span = slice(block * fb, (block + 1) * fb)
            pre = tuple(
                lax.dot_general(w[span], a, (((1,), (1,)), ((), ())), preferred_element_type=F32)
                for w, a in zip(weights, (tok, tok, cot))
            )
            act = jnp.stack(pointwise(*lax.psum(pre, "col")), 0)
        span = slice(block * fb, (block + 1) * fb)
        for k in range(2):
            term = lax.dot_general(
                act[k], weights[k][span], (((0,), (0,)), ((), ())), preferred_element_type=F32
            )
            total = term if total is None else total + term
        held = weight_grads(act, tok, cot, held, block, ff)
    grad_in = scatter_rows(total)
    return (grad_in.astype(BF), *held)


def solution(mesh):
    spec = P(("dp", "row"), "col")
    return jax.shard_map(
        shards,
        mesh=mesh,
        in_specs=(spec,) * 5,
        out_specs=(spec,) * 4,
        check_vma=False,
    )
```
